512 devices in a mesh: dom: 512 (over z, x, y, core).
Axes of the slice: x: 4, y: 8, z: 8, core: 2. Of those that a mesh axis runs over, the one named last changes fastest.
Arguments:
- tracers: float32 [20, 8, 524288], P(None, None, 'dom'), may hold values from -6 to 6
- mass_flux: float32 [3, 8, 524288], P(None, None, 'dom'), may hold values from -6 to 6
- lsq_coeff: float32 [2, 3, 524288], P(None, None, 'dom'), may hold values from -3 to 3
- own_offset: float32 [2, 3, 8, 524288], P(None, None, None, 'dom'), may hold values from -1.5 to 1.5
- far_offset: float32 [2, 3, 8, 524288], P(None, None, None, 'dom'), may hold values from -1.5 to 1.5
- inv_mass: float32 [8, 524288], P(None, 'dom'), may hold values from 0.25 to 1
- neighbour: int32 [3, 524288], P(None, 'dom'), may hold values from 0 to 1791, as said below
- send_cells: int32 [6, 65536], P(None, 'dom'), may hold values from 0 to 1023, as said below
Outputs:
- updated: float32 [20, 8, 524288], P(None, None, 'dom')
The draws below stay inside these ranges and needn't reach their ends.
Inputs may be any that keep to these rules, and one draw needn't show every extreme that they name: For each domain, entries index its 1024 own cells followed by 6 received blocks of 128 slots; every referenced received slot holds a real cell of the sending domain, the unused tail of a block is never referenced, and for every neighbour slot some domain references a block in full. `send_cells`: each block of 128 entries (one sending domain, one neighbour slot) lists distinct own cells of the sending domain, as local indices.
All inputs are finite; a program needn't handle non-finite values.
Results may differ from the reference program's by a relative error of at most 0.0003.
Values sent between devices are 32-bit elements; how exact they have to be, the bound alone decides.
A program may use at most 64 MiB of HBM per device.

```python
import math
import jax
import jax.numpy as jnp

TRC = 20
LEV = 8
CEL_DEV = 1024
PEERS = 6
HALO = 128
NCELL = 524288


def peer_shift_drawn(peer_slot):
    return (peer_slot // 2 + 1) * (1 - 2 * (peer_slot % 2))


def mesh_tables(key):
    devices = NCELL // CEL_DEV
    offsets = jnp.array([peer_shift_drawn(peer_slot) for peer_slot in range(PEERS)], jnp.int32)
    fewest = max(1, HALO // 4)
    counts = jax.random.randint(jax.random.fold_in(key, 101), (devices, PEERS), fewest, HALO + 1)
    full_rank = jax.random.randint(jax.random.fold_in(key, 102), (PEERS,), 0, devices)
    counts = jnp.where(jnp.arange(devices)[:, None] == full_rank[None, :], HALO, counts)
    send_keys = jax.random.split(jax.random.fold_in(key, 103), devices * PEERS)

    def pick_cells(subkey):
        return jax.random.permutation(subkey, CEL_DEV)[:HALO]
    chosen = jax.vmap(pick_cells)(send_keys)
    send_table = chosen.reshape(devices, PEERS, HALO).transpose(1, 0, 2).reshape(PEERS, devices * HALO)
    sender = (jnp.arange(devices)[:, None] - offsets[None, :]) % devices
    recv_counts = counts[sender, jnp.arange(PEERS)[None, :]]
    slot_range = jnp.arange(HALO)
    usable = slot_range[None, None, :] < recv_counts[:, :, None]
    values = CEL_DEV + jnp.arange(PEERS)[:, None] * HALO + slot_range[None, :]
    slot_table = jnp.where(usable, values[None], -1).reshape(devices, PEERS * HALO)
    filler = jnp.full((devices, 3 * CEL_DEV - PEERS * HALO), -1, slot_table.dtype)
    padded = jnp.concatenate([slot_table, filler], axis=1)
    place_keys = jax.random.split(jax.random.fold_in(key, 104), devices)

    def place_row(subkey, slot_row):
        return slot_row[jax.random.permutation(subkey, 3 * CEL_DEV)]
    placed = jax.vmap(place_row)(place_keys, padded).reshape(devices, 3, CEL_DEV)
    jumps = jax.random.randint(jax.random.fold_in(key, 105), (devices, 3, CEL_DEV), 1, CEL_DEV)
    local_pick = (jnp.arange(CEL_DEV)[None, None, :] + jumps) % CEL_DEV
    neighbour_table = jnp.where(placed >= 0, placed, local_pick).transpose(1, 0, 2).reshape(3, devices * CEL_DEV)
    return (neighbour_table.astype(jnp.int32), send_table.astype(jnp.int32))


def draw_neighbour(key, part):
    return mesh_tables(key)[0]


def draw_send_cells(key, part):
    return mesh_tables(key)[1]


def steps_of(own_key, extent, cuts, low, high):
    def one(position, blocks):
        draws = jax.random.uniform(jax.random.fold_in(jax.random.fold_in(own_key, 6), position), (blocks,), jnp.float32, low / len(cuts), high / len(cuts))
        return jnp.repeat(jnp.exp(draws), extent[position] // blocks).reshape((-1,) + (1,) * (len(extent) - position - 1))

    level = one(*cuts[0])
    for cut in cuts[1:]:
        level = level * one(*cut)
    return level


def noise(rng, dims, width, reach, cuts=(), held_as=jnp.bfloat16):
    result = width * jax.random.normal(rng, dims, jnp.float32)
    if cuts:
        result = result * steps_of(rng, dims, cuts, -0.22, 0.18)
    return jnp.clip(result, -reach, reach).astype(held_as)


def setup_inputs(seed: int = 0) -> dict:
    arg_keys = jax.random.split(jax.random.key(seed), 9)
    tracers = noise(arg_keys[0], (TRC, LEV, NCELL), 1.0, 6.0, ((2, 512),), jnp.float32)
    mass_flux = noise(arg_keys[1], (3, LEV, NCELL), 1.0, 6.0, ((2, 512),), jnp.float32)
    lsq_coeff = noise(arg_keys[2], (2, 3, NCELL), 0.5, 3.0, ((2, 512),), jnp.float32)
    own_offset = noise(arg_keys[3], (2, 3, LEV, NCELL), 0.3, 1.5, ((3, 512),), jnp.float32)
    far_offset = noise(arg_keys[4], (2, 3, LEV, NCELL), 0.3, 1.5, ((3, 512),), jnp.float32)
    inv_mass = jnp.clip(jnp.exp(math.log(1.0) - 1.3862944 * jax.random.uniform(arg_keys[5], (LEV, NCELL), jnp.float32) ** steps_of(arg_keys[5], (LEV, NCELL), ((1, 512),), -0.2, 0.2)), 0.25, 1.0)
    neighbour = draw_neighbour(jax.random.fold_in(arg_keys[8], 71), 0)
    send_cells = draw_send_cells(jax.random.fold_in(arg_keys[8], 71), 0)
    return {"tracers": tracers, "mass_flux": mass_flux, "lsq_coeff": lsq_coeff, "own_offset": own_offset, "far_offset": far_offset, "inv_mass": inv_mass, "neighbour": neighbour, "send_cells": send_cells}


def peer_shift(peer_slot):
    return (peer_slot // 2 + 1) * (1 - 2 * (peer_slot % 2))


def reference(tracers, mass_flux, lsq_coeff, own_offset, far_offset, inv_mass, neighbour, send_cells):
    devices = NCELL // CEL_DEV
    offsets = jnp.array([peer_shift(peer_slot) for peer_slot in range(PEERS)], jnp.int32)
    owners = jnp.arange(devices, dtype=jnp.int32)
    sender = ((owners[:, None] - offsets[None, :]) % devices).astype(jnp.int32)
    blocks = send_cells.reshape(PEERS, devices, HALO).astype(jnp.int32)
    remote = blocks[jnp.arange(PEERS, dtype=jnp.int32)[None, :], sender, :]
    remote = (remote + sender[:, :, None] * CEL_DEV).astype(jnp.int32)
    own_ids = (owners[:, None] * CEL_DEV + jnp.arange(CEL_DEV, dtype=jnp.int32)[None, :]).astype(jnp.int32)
    lookup = jnp.concatenate([own_ids, remote.reshape(devices, PEERS * HALO)], axis=1).astype(jnp.int32)
    local_ids = neighbour.reshape(3, devices, CEL_DEV).astype(jnp.int32)
    wide_lookup = jnp.broadcast_to(lookup[None], (3, devices, lookup.shape[1]))
    global_ids = jnp.take_along_axis(wide_lookup, local_ids, axis=2).reshape(3, NCELL).astype(jnp.int32)
    beside = [jnp.take(tracers, global_ids[edge_slot], axis=2) for edge_slot in range(3)]
    gradient = None
    for edge_slot in range(3):
        summand = lsq_coeff[:, edge_slot][:, None, None, :] * (beside[edge_slot] - tracers)[None]
        gradient = summand if gradient is None else gradient + summand
    outflow = jnp.zeros_like(tracers)
    for edge_slot in range(3):
        far_value = beside[edge_slot]
        far_grad = jnp.take(gradient, global_ids[edge_slot], axis=3)
        own_face = tracers + gradient[0] * own_offset[0, edge_slot] + gradient[1] * own_offset[1, edge_slot]
        far_face = far_value + far_grad[0] * far_offset[0, edge_slot] + far_grad[1] * far_offset[1, edge_slot]
        side_flux = mass_flux[edge_slot]
        face_value = jnp.where(side_flux > 0, own_face, far_face)
        face_value = jnp.clip(face_value, jnp.minimum(tracers, far_value), jnp.maximum(tracers, far_value))
        outflow = outflow + side_flux * face_value
    return tracers - inv_mass * outflow
```

```python
import functools

import jax
import jax.numpy as jnp
from jax import lax
from jax.experimental import pallas as pl
from jax.experimental.pallas import tpu as pltpu
from jax.sharding import PartitionSpec as P

LANES = 128
CHUNKS = 4


def peer_shift(peer_slot):
    return (peer_slot // 2 + 1) * (1 - 2 * (peer_slot % 2))


def lanes_of(row):
    wide = jnp.broadcast_to(row, (8, LANES))
    return jnp.bitwise_and(wide, LANES - 1), jnp.right_shift(wide, 7)


def taken(tile, lane):
    return jnp.take_along_axis(tile, lane, axis=1, mode="promise_in_bounds")


def kernel(
    device_count,
    x_any, flux_any, lsq_any, own_any, far_any, inv_any, near_any, send_any,
    out_any,
    x, flux, lsq, own, far, inv, near, send,
    value_out, value_in, grad_out, grad_in, grad, beside, early, result,
    load_sem, store_sem, value_send, value_recv, grad_send, grad_recv,
):
    me = lax.axis_index("dom")
    tracer_count, level_count, cell_count = x.shape
    peer_count = send.shape[0]
    tiles = cell_count // LANES
    step = tracer_count // CHUNKS
    targets = [
        lax.rem(me + peer_shift(slot) + device_count, device_count)
        for slot in range(peer_count)
    ]

    loads = []
    for slot, (source, target) in enumerate((
        (send_any, send), (x_any, x), (near_any, near), (lsq_any, lsq),
        (flux_any, flux), (own_any, own), (far_any, far), (inv_any, inv),
    )):
        copy = pltpu.make_async_copy(source, target, load_sem.at[slot])
        copy.start()
        loads.append(copy)

    barrier = pltpu.get_barrier_semaphore()
    for target in targets:
        pl.semaphore_signal(
            barrier, inc=1, device_id=(target,), device_id_type=pl.DeviceIdType.MESH
        )

    def cut(tile):
        return slice(tile * LANES, (tile + 1) * LANES)

    def value_copy(slot, chunk):
        part = pl.ds(chunk * step, step)
        return pltpu.make_async_remote_copy(
            src_ref=value_out.at[slot, part],
            dst_ref=value_in.at[slot, part],
            send_sem=value_send.at[slot, chunk],
            recv_sem=value_recv.at[slot, chunk],
            device_id=(targets[slot],),
            device_id_type=pl.DeviceIdType.MESH,
        )

    def grad_copy(slot, chunk):
        part = pl.ds(chunk * step, step)
        return pltpu.make_async_remote_copy(
            src_ref=grad_out.at[slot, part],
            dst_ref=grad_in.at[slot, part],
            send_sem=grad_send.at[slot, chunk],
            recv_sem=grad_recv.at[slot, chunk],
            device_id=(targets[slot],),
            device_id_type=pl.DeviceIdType.MESH,
        )

    def gather_values_to_send(chunk):
        for slot in range(peer_count):
            lane, tile = lanes_of(send[slot : slot + 1, :])
            for inner in range(step):
                t = chunk * step + inner
                found = taken(x[t, :, cut(0)], lane)
                for s in range(1, tiles):
                    found = jnp.where(tile == s, taken(x[t, :, cut(s)], lane), found)
                value_out[slot, t] = found

    def gather_own_values(chunk):
        for edge in range(3):
            for c in range(tiles):
                lane, tile = lanes_of(near[edge : edge + 1, cut(c)])
                for inner in range(step):
                    t = chunk * step + inner
                    found = taken(x[t, :, cut(0)], lane)
                    for s in range(1, tiles):
                        found = jnp.where(tile == s, taken(x[t, :, cut(s)], lane), found)
                    beside[edge, t, :, cut(c)] = found

    def make_gradients(chunk):
        for c in range(tiles):
            for inner in range(step):
                t = chunk * step + inner
                here = x[t, :, cut(c)]
                total = [None, None]
                for edge in range(3):
                    lane, tile = lanes_of(near[edge : edge + 1, cut(c)])
                    found = beside[edge, t, :, cut(c)]
                    for slot in range(peer_count):
                        found = jnp.where(
                            tile == tiles + slot, taken(value_in[slot, t], lane), found
                        )
                    beside[edge, t, :, cut(c)] = found
                    gap = found - here
                    for comp in range(2):
                        term = lsq[comp, edge : edge + 1, cut(c)] * gap
                        total[comp] = term if edge == 0 else total[comp] + term
                for comp in range(2):
                    grad[comp, t, :, cut(c)] = total[comp]

    def gather_gradients_to_send(chunk):
        for slot in range(peer_count):
            lane, tile = lanes_of(send[slot : slot + 1, :])
            for inner in range(step):
                t = chunk * step + inner
                for comp in range(2):
                    found = taken(grad[comp, t, :, cut(0)], lane)
                    for s in range(1, tiles):
                        found = jnp.where(
                            tile == s, taken(grad[comp, t, :, cut(s)], lane), found
                        )
                    grad_out[slot, t, comp] = found

    def make_early_faces(chunk):
        for edge in range(3):
            for c in range(tiles):
                lane, tile = lanes_of(near[edge : edge + 1, cut(c)])
                upwind = flux[edge, :, cut(c)] > 0
                for inner in range(step):
                    t = chunk * step + inner
                    slopes = []
                    for comp in range(2):
                        found = taken(grad[comp, t, :, cut(0)], lane)
                        for s in range(1, tiles):
                            found = jnp.where(
                                tile == s, taken(grad[comp, t, :, cut(s)], lane), found
                            )
                        slopes.append(found)
                    far_face = (
                        beside[edge, t, :, cut(c)]
                        + slopes[0] * far[0, edge, :, cut(c)]
                        + slopes[1] * far[1, edge, :, cut(c)]
                    )
                    own_face = (
                        x[t, :, cut(c)]
                        + grad[0, t, :, cut(c)] * own[0, edge, :, cut(c)]
                        + grad[1, t, :, cut(c)] * own[1, edge, :, cut(c)]
                    )
                    early[edge, t, :, cut(c)] = jnp.where(upwind, own_face, far_face)

    def finish(chunk):
        for c in range(tiles):
            for inner in range(step):
                t = chunk * step + inner
                here = x[t, :, cut(c)]
                outflow = None
                for edge in range(3):
                    lane, tile = lanes_of(near[edge : edge + 1, cut(c)])
                    side_flux = flux[edge, :, cut(c)]
                    late = jnp.logical_and(tile >= tiles, jnp.logical_not(side_flux > 0))
                    beyond = beside[edge, t, :, cut(c)]
                    slopes = []
                    for comp in range(2):
                        found = taken(grad_in[0, t, comp], lane)
                        for slot in range(1, peer_count):
                            found = jnp.where(
                                tile == tiles + slot, taken(grad_in[slot, t, comp], lane), found
                            )
                        slopes.append(found)
                    far_face = (
                        beyond
                        + slopes[0] * far[0, edge, :, cut(c)]
                        + slopes[1] * far[1, edge, :, cut(c)]
                    )
                    face = jnp.where(late, far_face, early[edge, t, :, cut(c)])
                    face = jnp.minimum(
                        jnp.maximum(face, jnp.minimum(here, beyond)), jnp.maximum(here, beyond)
                    )
                    term = side_flux * face
                    outflow = term if edge == 0 else outflow + term
                result[t, :, cut(c)] = here - inv[:, cut(c)] * outflow

    def over_chunks(body):
        lax.fori_loop(0, CHUNKS, lambda chunk, carry: (body(chunk), carry)[1], 0)

    loads[0].wait()
    loads[1].wait()
    over_chunks(gather_values_to_send)
    pl.semaphore_wait(barrier, peer_count)
    for chunk in range(CHUNKS):
        for slot in range(peer_count):
            value_copy(slot, chunk).start()
    for copy in loads[2:]:
        copy.wait()
    over_chunks(gather_own_values)

    def middle(chunk):
        for slot in range(peer_count):
            value_copy(slot, chunk).wait_recv()
        make_gradients(chunk)
        gather_gradients_to_send(chunk)
        for slot in range(peer_count):
            grad_copy(slot, chunk).start()

    over_chunks(middle)
    over_chunks(make_early_faces)

    def store(chunk):
        part = pl.ds(chunk * step, step)
        return pltpu.make_async_copy(result.at[part], out_any.at[part], store_sem.at[chunk])

    def last(chunk):
        for slot in range(peer_count):
            grad_copy(slot, chunk).wait_recv()
        finish(chunk)
        store(chunk).start()

    over_chunks(last)
    for chunk in range(CHUNKS):
        for slot in range(peer_count):
            value_copy(slot, chunk).wait_send()
            grad_copy(slot, chunk).wait_send()
        store(chunk).wait()


def on_device(
    device_count,
    tracers, mass_flux, lsq_coeff, own_offset, far_offset, inv_mass, neighbour, send_cells,
):
    tracer_count, level_count, cell_count = tracers.shape
    peer_count, halo_width = send_cells.shape
    f32 = jnp.float32
    arguments = (
        tracers, mass_flux, lsq_coeff, own_offset, far_offset, inv_mass, neighbour, send_cells,
    )
    halo = (peer_count, tracer_count, level_count, halo_width)
    halo_two = (peer_count, tracer_count, 2, level_count, halo_width)
    return pl.pallas_call(
        functools.partial(kernel, device_count),
        out_shape=jax.ShapeDtypeStruct(tracers.shape, f32),
        in_specs=[pl.BlockSpec(memory_space=pltpu.HBM)] * len(arguments),
        out_specs=pl.BlockSpec(memory_space=pltpu.HBM),
        scratch_shapes=[pltpu.VMEM(a.shape, a.dtype) for a in arguments]
        + [
            pltpu.VMEM(halo, f32),
            pltpu.VMEM(halo, f32),
            pltpu.VMEM(halo_two, f32),
            pltpu.VMEM(halo_two, f32),
            pltpu.VMEM((2, tracer_count, level_count, cell_count), f32),
            pltpu.VMEM((3, tracer_count, level_count, cell_count), f32),
            pltpu.VMEM((3, tracer_count, level_count, cell_count), f32),
            pltpu.VMEM(tracers.shape, f32),
            pltpu.SemaphoreType.DMA((len(arguments),)),
            pltpu.SemaphoreType.DMA((CHUNKS,)),
            pltpu.SemaphoreType.DMA((peer_count, CHUNKS)),
            pltpu.SemaphoreType.DMA((peer_count, CHUNKS)),
            pltpu.SemaphoreType.DMA((peer_count, CHUNKS)),
            pltpu.SemaphoreType.DMA((peer_count, CHUNKS)),
        ],
        compiler_params=pltpu.CompilerParams(collective_id=0, has_side_effects=True),
    )(*arguments)


def solution(mesh):
    placed = (
        P(None, None, "dom"),
        P(None, None, "dom"),
        P(None, None, "dom"),
        P(None, None, None, "dom"),
        P(None, None, None, "dom"),
        P(None, "dom"),
        P(None, "dom"),
        P(None, "dom"),
    )
    return jax.shard_map(
        functools.partial(on_device, mesh.shape["dom"]),
        mesh=mesh,
        in_specs=placed,
        out_specs=P(None, None, "dom"),
        check_vma=False,
    )
```

```python
import functools

import jax
import jax.numpy as jnp
from jax import lax
from jax.experimental import pallas as pl
from jax.experimental.pallas import tpu as pltpu
from jax.sharding import PartitionSpec as P

LANES = 128
CHUNKS = 4
BLOCK = 256


def peer_shift(peer_slot):
    return (peer_slot // 2 + 1) * (1 - 2 * (peer_slot % 2))


def lanes_of(row):
    wide = jnp.broadcast_to(row, (8, LANES))
    return jnp.bitwise_and(wide, LANES - 1), jnp.right_shift(wide, 7)


def taken(tile, lane):
    return jnp.take_along_axis(tile, lane, axis=1, mode="promise_in_bounds")


def in_two(value):
    high = value.astype(jnp.bfloat16)
    return high, (value - high.astype(jnp.float32)).astype(jnp.bfloat16)


def kernel(
    device_count,
    x_any, flux_any, lsq_any, own_any, far_any, inv_any, near_any, send_any,
    out_any,
    x, flux, lsq, own, far, inv, near, send,
    value_out, value_in, grad_out, grad_in, grad, beside, early, result,
    own_hot, halo_hot, value_split, grad_split, halo_split,
    load_sem, store_sem, value_send, value_recv, grad_send, grad_recv,
):
    me = lax.axis_index("dom")
    tracer_count, level_count, cell_count = x.shape
    peer_count = send.shape[0]
    tiles = cell_count // LANES
    step = tracer_count // CHUNKS
    targets = [
        lax.rem(me + peer_shift(slot) + device_count, device_count)
        for slot in range(peer_count)
    ]

    loads = []
    for slot, (source, target) in enumerate((
        (send_any, send), (x_any, x), (near_any, near), (lsq_any, lsq),
        (flux_any, flux), (own_any, own), (far_any, far), (inv_any, inv),
    )):
        copy = pltpu.make_async_copy(source, target, load_sem.at[slot])
        copy.start()
        loads.append(copy)

    barrier = pltpu.get_barrier_semaphore()
    for target in targets:
        pl.semaphore_signal(
            barrier, inc=1, device_id=(target,), device_id_type=pl.DeviceIdType.MESH
        )

    def cut(tile):
        return slice(tile * LANES, (tile + 1) * LANES)

    def value_copy(slot, chunk):
        part = pl.ds(chunk * step, step)
        return pltpu.make_async_remote_copy(
            src_ref=value_out.at[slot, part],
            dst_ref=value_in.at[slot, part],
            send_sem=value_send.at[slot, chunk],
            recv_sem=value_recv.at[slot, chunk],
            device_id=(targets[slot],),
            device_id_type=pl.DeviceIdType.MESH,
        )

    def grad_copy(slot, chunk):
        part = pl.ds(chunk * step, step)
        return pltpu.make_async_remote_copy(
            src_ref=grad_out.at[slot, part],
            dst_ref=grad_in.at[slot, part],
            send_sem=grad_send.at[slot, chunk],
            recv_sem=grad_recv.at[slot, chunk],
            device_id=(targets[slot],),
            device_id_type=pl.DeviceIdType.MESH,
        )

    def gather_values_to_send(chunk):
        for slot in range(peer_count):
            lane, tile = lanes_of(send[slot : slot + 1, :])
            for inner in range(step):
                t = chunk * step + inner
                found = taken(x[t, :, cut(0)], lane)
                for s in range(1, tiles):
                    found = jnp.where(tile == s, taken(x[t, :, cut(s)], lane), found)
                value_out[slot, t] = found

    def split_values():
        for t in range(0, tracer_count, 2):
            rows = slice(t * level_count, (t + 2) * level_count)
            for c in range(tiles):
                pair = jnp.concatenate([x[t, :, cut(c)], x[t + 1, :, cut(c)]], axis=0)
                for part, half in enumerate(in_two(pair)):
                    value_split[part, rows, cut(c)] = half

    def mark(hot, first):
        depth = hot.shape[0]
        for edge in range(3):
            wanted = near[edge : edge + 1, :] - first
            for k in range(0, depth, 256):
                row = lax.broadcasted_iota(jnp.int32, (256, cell_count), 0) + k
                hot[k : k + 256, edge * cell_count : (edge + 1) * cell_count] = jnp.where(
                    row == wanted, 1.0, 0.0
                ).astype(jnp.bfloat16)

    def gathered(split, hot, edge, block):
        rows = split.shape[1]
        both = split[...].reshape(2 * rows, split.shape[2])
        columns = pl.ds(
            pl.multiple_of(edge * cell_count + block * BLOCK, BLOCK), BLOCK
        )
        found = jnp.dot(both, hot[:, columns], preferred_element_type=jnp.float32)
        return found[:rows] + found[rows:]

    def gather_own_values(edge):
        for block in range(cell_count // BLOCK):
            found = gathered(value_split, own_hot, edge, block)
            beside[edge, :, :, slice(block * BLOCK, (block + 1) * BLOCK)] = found.reshape(
                tracer_count, level_count, BLOCK
            )

    def make_gradients(chunk):
        for c in range(tiles):
            for inner in range(step):
                t = chunk * step + inner
                here = x[t, :, cut(c)]
                total = [None, None]
                for edge in range(3):
                    lane, tile = lanes_of(near[edge : edge + 1, cut(c)])
                    found = beside[edge, t, :, cut(c)]
                    for slot in range(peer_count):
                        found = jnp.where(
                            tile == tiles + slot, taken(value_in[slot, t], lane), found
                        )
                    beside[edge, t, :, cut(c)] = found
                    gap = found - here
                    for comp in range(2):
                        term = lsq[edge, comp : comp + 1, cut(c)] * gap
                        total[comp] = term if edge == 0 else total[comp] + term
                for comp in range(2):
                    grad[comp, t, :, cut(c)] = total[comp]
                rows = pl.ds(pl.multiple_of(t * 2 * level_count, 2 * level_count), 2 * level_count)
                for part, half in enumerate(in_two(jnp.concatenate(total, axis=0))):
                    grad_split[part, rows, cut(c)] = half

    def gather_gradients_to_send(chunk):
        for slot in range(peer_count):
            lane, tile = lanes_of(send[slot : slot + 1, :])
            for inner in range(step):
                t = chunk * step + inner
                for comp in range(2):
                    found = taken(grad[comp, t, :, cut(0)], lane)
                    for s in range(1, tiles):
                        found = jnp.where(
                            tile == s, taken(grad[comp, t, :, cut(s)], lane), found
                        )
                    grad_out[slot, t, comp] = found

    def make_early_faces(edge):
        for block in range(cell_count // BLOCK):
            found = gathered(grad_split, own_hot, edge, block)
            here = slice(block * BLOCK, (block + 1) * BLOCK)
            upwind = flux[edge, :, here] > 0
            for t in range(tracer_count):
                top = t * 2 * level_count
                first = found[top : top + level_count]
                second = found[top + level_count : top + 2 * level_count]
                far_face = (
                    beside[edge, t, :, here]
                    + first * far[0, edge, :, here]
                    + second * far[1, edge, :, here]
                )
                own_face = (
                    x[t, :, here]
                    + grad[0, t, :, here] * own[0, edge, :, here]
                    + grad[1, t, :, here] * own[1, edge, :, here]
                )
                early[edge, t, :, here] = jnp.where(upwind, own_face, far_face)

    def add_halo_faces(chunk):
        for inner in range(step):
            t = chunk * step + inner
            rows = slice(inner * 2 * level_count, (inner + 1) * 2 * level_count)
            for slot in range(peer_count):
                pair = grad_in[slot, t].reshape(2 * level_count, LANES)
                for part, half in enumerate(in_two(pair)):
                    halo_split[part, rows, cut(slot)] = half
        for block in range(cell_count // BLOCK):
            here = slice(block * BLOCK, (block + 1) * BLOCK)
            slopes = [gathered(halo_split, halo_hot, edge, block) for edge in range(3)]
            for inner in range(step):
                t = chunk * step + inner
                top = inner * 2 * level_count
                center = x[t, :, here]
                outflow = None
                for edge in range(3):
                    first = slopes[edge][top : top + level_count]
                    second = slopes[edge][top + level_count : top + 2 * level_count]
                    side_flux = flux[edge, :, here]
                    beyond = beside[edge, t, :, here]
                    extra = first * far[0, edge, :, here] + second * far[1, edge, :, here]
                    face = early[edge, t, :, here] + jnp.where(side_flux > 0, 0.0, extra)
                    face = jnp.minimum(
                        jnp.maximum(face, jnp.minimum(center, beyond)),
                        jnp.maximum(center, beyond),
                    )
                    term = side_flux * face
                    outflow = term if edge == 0 else outflow + term
                result[t, :, here] = center - inv[:, here] * outflow

    def finish(chunk):
        for c in range(tiles):
            for inner in range(step):
                t = chunk * step + inner
                here = x[t, :, cut(c)]
                outflow = None
                for edge in range(3):
                    lane, tile = lanes_of(near[edge : edge + 1, cut(c)])
                    side_flux = flux[edge, :, cut(c)]
                    late = jnp.logical_and(tile >= tiles, jnp.logical_not(side_flux > 0))
                    beyond = beside[edge, t, :, cut(c)]
                    slopes = []
                    for comp in range(2):
                        found = taken(grad_in[0, t, comp], lane)
                        for slot in range(1, peer_count):
                            found = jnp.where(
                                tile == tiles + slot, taken(grad_in[slot, t, comp], lane), found
                            )
                        slopes.append(found)
                    far_face = (
                        beyond
                        + slopes[0] * far[0, edge, :, cut(c)]
                        + slopes[1] * far[1, edge, :, cut(c)]
                    )
                    face = jnp.where(late, far_face, early[edge, t, :, cut(c)])
                    face = jnp.minimum(
                        jnp.maximum(face, jnp.minimum(here, beyond)), jnp.maximum(here, beyond)
                    )
                    term = side_flux * face
                    outflow = term if edge == 0 else outflow + term
                result[t, :, cut(c)] = here - inv[:, cut(c)] * outflow

    def over(count, body):
        lax.fori_loop(0, count, lambda index, carry: (body(index), carry)[1], 0)

    loads[0].wait()
    loads[1].wait()
    gather_values_to_send(0)
    pl.semaphore_wait(barrier, peer_count)

    def send_values(chunk):
        for slot in range(peer_count):
            value_copy(slot, chunk).start()

    send_values(0)

    def next_values(before):
        gather_values_to_send(before + 1)
        send_values(before + 1)

    over(CHUNKS - 1, next_values)
    for copy in loads[2:]:
        copy.wait()
    split_values()
    mark(own_hot, 0)
    over(3, gather_own_values)
    mark(halo_hot, cell_count)

    def middle(chunk):
        for slot in range(peer_count):
            value_copy(slot, chunk).wait_recv()
        make_gradients(chunk)
        gather_gradients_to_send(chunk)
        for slot in range(peer_count):
            grad_copy(slot, chunk).start()

    over(CHUNKS, middle)
    over(3, make_early_faces)

    def store(chunk):
        part = pl.ds(chunk * step, step)
        return pltpu.make_async_copy(result.at[part], out_any.at[part], store_sem.at[chunk])

    def last(chunk, complete):
        for slot in range(peer_count):
            grad_copy(slot, chunk).wait_recv()
        complete(chunk)
        store(chunk).start()

    over(CHUNKS - 1, lambda chunk: last(chunk, add_halo_faces))
    last(CHUNKS - 1, finish)
    for chunk in range(CHUNKS):
        for slot in range(peer_count):
            value_copy(slot, chunk).wait_send()
            grad_copy(slot, chunk).wait_send()
        store(chunk).wait()


def on_device(
    device_count,
    tracers, mass_flux, lsq_coeff, own_offset, far_offset, inv_mass, neighbour, send_cells,
):
    tracer_count, level_count, cell_count = tracers.shape
    peer_count, halo_width = send_cells.shape
    f32, bf16 = jnp.float32, jnp.bfloat16
    arguments = (
        tracers, mass_flux, lsq_coeff.transpose(1, 0, 2), own_offset, far_offset, inv_mass,
        neighbour, send_cells,
    )
    halo = (peer_count, tracer_count, level_count, halo_width)
    halo_two = (peer_count, tracer_count, 2, level_count, halo_width)
    return pl.pallas_call(
        functools.partial(kernel, device_count),
        out_shape=jax.ShapeDtypeStruct(tracers.shape, f32),
        in_specs=[pl.BlockSpec(memory_space=pltpu.HBM)] * len(arguments),
        out_specs=pl.BlockSpec(memory_space=pltpu.HBM),
        scratch_shapes=[pltpu.VMEM(a.shape, a.dtype) for a in arguments]
        + [
            pltpu.VMEM(halo, f32),
            pltpu.VMEM(halo, f32),
            pltpu.VMEM(halo_two, f32),
            pltpu.VMEM(halo_two, f32),
            pltpu.VMEM((2, tracer_count, level_count, cell_count), f32),
            pltpu.VMEM((3, tracer_count, level_count, cell_count), f32),
            pltpu.VMEM((3, tracer_count, level_count, cell_count), f32),
            pltpu.VMEM(tracers.shape, f32),
            pltpu.VMEM((cell_count, 3 * cell_count), bf16),
            pltpu.VMEM((peer_count * halo_width, 3 * cell_count), bf16),
            pltpu.VMEM((2, tracer_count * level_count, cell_count), bf16),
            pltpu.VMEM((2, tracer_count * 2 * level_count, cell_count), bf16),
            pltpu.VMEM((2, tracer_count // CHUNKS * 2 * level_count, peer_count * halo_width), bf16),
            pltpu.SemaphoreType.DMA((len(arguments),)),
            pltpu.SemaphoreType.DMA((CHUNKS,)),
            pltpu.SemaphoreType.DMA((peer_count, CHUNKS)),
            pltpu.SemaphoreType.DMA((peer_count, CHUNKS)),
            pltpu.SemaphoreType.DMA((peer_count, CHUNKS)),
            pltpu.SemaphoreType.DMA((peer_count, CHUNKS)),
        ],
        compiler_params=pltpu.CompilerParams(collective_id=0, has_side_effects=True),
    )(*arguments)


def solution(mesh):
    placed = (
        P(None, None, "dom"),
        P(None, None, "dom"),
        P(None, None, "dom"),
        P(None, None, None, "dom"),
        P(None, None, None, "dom"),
        P(None, "dom"),
        P(None, "dom"),
        P(None, "dom"),
    )
    return jax.shard_map(
        functools.partial(on_device, mesh.shape["dom"]),
        mesh=mesh,
        in_specs=placed,
        out_specs=P(None, None, "dom"),
        check_vma=False,
    )
```

```python
import functools

import jax
import jax.numpy as jnp
from jax import lax
from jax.experimental import pallas as pl
from jax.experimental.pallas import tpu as pltpu
from jax.sharding import PartitionSpec as P

LANES = 128
BLOCK = 256
PARTS = (2, 4, 6, 5, 3)
JOINED = ((0, 1), (2,), (3,))
ORDER = (4, 5, 2, 3, 0, 1)


def peer_shift(peer_slot):
    return (peer_slot // 2 + 1) * (1 - 2 * (peer_slot % 2))


def lanes_of(row):
    wide = jnp.broadcast_to(row, (8, LANES))
    return jnp.bitwise_and(wide, LANES - 1), jnp.right_shift(wide, 7)


def taken(tile, lane):
    return jnp.take_along_axis(tile, lane, axis=1, mode="promise_in_bounds")


def in_two(value):
    high = value.astype(jnp.bfloat16)
    return high, (value - high.astype(jnp.float32)).astype(jnp.bfloat16)


def kernel(
    device_count,
    x_any, flux_any, lsq_any, own_any, far_any, inv_any, near_any, send_any,
    result,
    x, flux, lsq, own, far, inv, near, send,
    value_out, value_in, grad_out, grad_in, grad, beside, early,
    own_hot, halo_hot, value_split, grad_split, halo_split,
    load_sem, value_send, value_recv, grad_send, grad_recv,
):
    me = lax.axis_index("dom")
    tracer_count, level_count, cell_count = x.shape
    peer_count = send.shape[0]
    tiles = cell_count // LANES
    starts = [sum(PARTS[:chunk]) for chunk in range(len(PARTS) + 1)]
    targets = [
        lax.rem(me + peer_shift(slot) + device_count, device_count)
        for slot in range(peer_count)
    ]

    loads = []
    for slot, (source, target) in enumerate((
        (near_any, near), (send_any, send), (x_any, x), (lsq_any, lsq),
        (flux_any, flux), (own_any, own), (far_any, far), (inv_any, inv),
    )):
        copy = pltpu.make_async_copy(source, target, load_sem.at[slot])
        copy.start()
        loads.append(copy)

    barrier = pltpu.get_barrier_semaphore()
    for target in targets:
        pl.semaphore_signal(
            barrier, inc=1, device_id=(target,), device_id_type=pl.DeviceIdType.MESH
        )

    def cut(tile):
        return slice(tile * LANES, (tile + 1) * LANES)

    def value_copy(slot, chunk):
        part = pl.ds(starts[chunk], PARTS[chunk])
        return pltpu.make_async_remote_copy(
            src_ref=value_out.at[slot, part],
            dst_ref=value_in.at[slot, part],
            send_sem=value_send.at[slot, chunk],
            recv_sem=value_recv.at[slot, chunk],
            device_id=(targets[slot],),
            device_id_type=pl.DeviceIdType.MESH,
        )

    def grad_copy(slot, chunk):
        part = pl.ds(starts[chunk], PARTS[chunk])
        return pltpu.make_async_remote_copy(
            src_ref=grad_out.at[slot, part],
            dst_ref=grad_in.at[slot, part],
            send_sem=grad_send.at[slot, chunk],
            recv_sem=grad_recv.at[slot, chunk],
            device_id=(targets[slot],),
            device_id_type=pl.DeviceIdType.MESH,
        )

    def gather_values_to_send(chunk):
        for slot in range(peer_count):
            lane, tile = lanes_of(send[slot : slot + 1, :])
            for t in range(starts[chunk], starts[chunk + 1]):
                found = taken(x[t, :, cut(0)], lane)
                for s in range(1, tiles):
                    found = jnp.where(tile == s, taken(x[t, :, cut(s)], lane), found)
                value_out[slot, t] = found

    def split_values():
        for t in range(0, tracer_count, 2):
            rows = slice(t * level_count, (t + 2) * level_count)
            for c in range(tiles):
                pair = jnp.concatenate([x[t, :, cut(c)], x[t + 1, :, cut(c)]], axis=0)
                for part, half in enumerate(in_two(pair)):
                    value_split[part, rows, cut(c)] = half

    def mark(hot, first):
        depth = hot.shape[0]
        for edge in range(3):
            wanted = (near[edge : edge + 1, :] - first).astype(jnp.int16)
            for k in range(0, depth, 256):
                row = lax.broadcasted_iota(jnp.int16, (256, cell_count), 0) + jnp.int16(k)
                hot[k : k + 256, edge * cell_count : (edge + 1) * cell_count] = jnp.where(
                    row == wanted, jnp.bfloat16(1), jnp.bfloat16(0)
                )

    def gathered(split, rows, hot, edge, block):
        both = jnp.concatenate([split[0, :rows], split[1, :rows]], axis=0)
        first = edge * cell_count + block * BLOCK
        columns = pl.ds(pl.multiple_of(first, BLOCK), BLOCK)
        found = jnp.dot(both, hot[:, columns], preferred_element_type=jnp.float32)
        return found[:rows] + found[rows:]

    def gather_own_values(edge):
        for block in range(cell_count // BLOCK):
            found = gathered(value_split, value_split.shape[1], own_hot, edge, block)
            beside[edge, :, :, slice(block * BLOCK, (block + 1) * BLOCK)] = found.reshape(
                tracer_count, level_count, BLOCK
            )

    def make_gradients(chunk):
        for c in range(tiles):
            for t in range(starts[chunk], starts[chunk + 1]):
                here = x[t, :, cut(c)]
                total = [None, None]
                for edge in range(3):
                    lane, tile = lanes_of(near[edge : edge + 1, cut(c)])
                    found = beside[edge, t, :, cut(c)]
                    for slot in range(peer_count):
                        found = jnp.where(
                            tile == tiles + slot, taken(value_in[slot, t], lane), found
                        )
                    beside[edge, t, :, cut(c)] = found
                    gap = found - here
                    for comp in range(2):
                        term = lsq[edge, comp : comp + 1, cut(c)] * gap
                        total[comp] = term if edge == 0 else total[comp] + term
                for comp in range(2):
                    grad[comp, t, :, cut(c)] = total[comp]
                rows = slice(t * 2 * level_count, (t + 1) * 2 * level_count)
                for part, half in enumerate(in_two(jnp.concatenate(total, axis=0))):
                    grad_split[part, rows, cut(c)] = half

    def gather_gradients_to_send(chunk):
        for slot in range(peer_count):
            lane, tile = lanes_of(send[slot : slot + 1, :])
            for t in range(starts[chunk], starts[chunk + 1]):
                for comp in range(2):
                    found = taken(grad[comp, t, :, cut(0)], lane)
                    for s in range(1, tiles):
                        found = jnp.where(
                            tile == s, taken(grad[comp, t, :, cut(s)], lane), found
                        )
                    grad_out[slot, t, comp] = found

    def make_early_faces(edge):
        for block in range(cell_count // BLOCK):
            found = gathered(grad_split, grad_split.shape[1], own_hot, edge, block)
            here = slice(block * BLOCK, (block + 1) * BLOCK)
            upwind = flux[edge, :, here] > 0
            for t in range(tracer_count):
                top = t * 2 * level_count
                first = found[top : top + level_count]
                second = found[top + level_count : top + 2 * level_count]
                far_face = (
                    beside[edge, t, :, here]
                    + first * far[0, edge, :, here]
                    + second * far[1, edge, :, here]
                )
                own_face = (
                    x[t, :, here]
                    + grad[0, t, :, here] * own[0, edge, :, here]
                    + grad[1, t, :, here] * own[1, edge, :, here]
                )
                early[edge, t, :, here] = jnp.where(upwind, own_face, far_face)

    def add_halo_faces(first_tracer, count, blocks):
        for inner in range(count):
            rows = slice(inner * 2 * level_count, (inner + 1) * 2 * level_count)
            for slot in range(peer_count):
                pair = grad_in[slot, first_tracer + inner].reshape(2 * level_count, LANES)
                for part, half in enumerate(in_two(pair)):
                    halo_split[part, rows, cut(slot)] = half
        for block in blocks:
            here = slice(block * BLOCK, (block + 1) * BLOCK)
            slopes = [
                gathered(halo_split, count * 2 * level_count, halo_hot, edge, block)
                for edge in range(3)
            ]
            for inner in range(count):
                t = first_tracer + inner
                top = inner * 2 * level_count
                center = x[t, :, here]
                outflow = None
                for edge in range(3):
                    first = slopes[edge][top : top + level_count]
                    second = slopes[edge][top + level_count : top + 2 * level_count]
                    side_flux = flux[edge, :, here]
                    beyond = beside[edge, t, :, here]
                    extra = first * far[0, edge, :, here] + second * far[1, edge, :, here]
                    face = early[edge, t, :, here] + jnp.where(side_flux > 0, 0.0, extra)
                    face = jnp.minimum(
                        jnp.maximum(face, jnp.minimum(center, beyond)),
                        jnp.maximum(center, beyond),
                    )
                    term = side_flux * face
                    outflow = term if edge == 0 else outflow + term
                result[t, :, here] = center - inv[:, here] * outflow

    def finish(chunk, columns):
        for c in columns:
            for t in range(starts[chunk], starts[chunk + 1]):
                here = x[t, :, cut(c)]
                outflow = None
                for edge in range(3):
                    lane, tile = lanes_of(near[edge : edge + 1, cut(c)])
                    side_flux = flux[edge, :, cut(c)]
                    late = jnp.logical_and(tile >= tiles, jnp.logical_not(side_flux > 0))
                    beyond = beside[edge, t, :, cut(c)]
                    slopes = []
                    for comp in range(2):
                        found = taken(grad_in[0, t, comp], lane)
                        for slot in range(1, peer_count):
                            found = jnp.where(
                                tile == tiles + slot, taken(grad_in[slot, t, comp], lane), found
                            )
                        slopes.append(found)
                    far_face = (
                        beyond
                        + slopes[0] * far[0, edge, :, cut(c)]
                        + slopes[1] * far[1, edge, :, cut(c)]
                    )
                    face = jnp.where(late, far_face, early[edge, t, :, cut(c)])
                    face = jnp.minimum(
                        jnp.maximum(face, jnp.minimum(here, beyond)), jnp.maximum(here, beyond)
                    )
                    term = side_flux * face
                    outflow = term if edge == 0 else outflow + term
                result[t, :, cut(c)] = here - inv[:, cut(c)] * outflow

    def over(count, body):
        lax.fori_loop(0, count, lambda index, carry: (body(index), carry)[1], 0)

    chunks = range(len(PARTS))
    loads[0].wait()
    mark(own_hot, 0)
    loads[1].wait()
    loads[2].wait()
    gather_values_to_send(0)
    pl.semaphore_wait(barrier, peer_count)
    for chunk in chunks:
        if chunk > 0:
            gather_values_to_send(chunk)
        for slot in ORDER:
            value_copy(slot, chunk).start()
    for copy in loads[3:]:
        copy.wait()
    split_values()
    over(3, gather_own_values)
    for chunk in chunks:
        for slot in ORDER:
            value_copy(slot, chunk).wait_recv()
        make_gradients(chunk)
        gather_gradients_to_send(chunk)
        for slot in ORDER:
            grad_copy(slot, chunk).start()
    mark(halo_hot, cell_count)
    over(3, make_early_faces)
    blocks = range(cell_count // BLOCK)
    for joined in JOINED:
        for chunk in joined:
            for slot in ORDER:
                grad_copy(slot, chunk).wait_recv()
        count = sum(PARTS[chunk] for chunk in joined)
        add_halo_faces(starts[joined[0]], count, blocks)
    final = len(PARTS) - 1
    for slot in ORDER:
        grad_copy(slot, final).wait_recv()
    add_halo_faces(starts[final], PARTS[final], blocks[: len(blocks) // 2])
    finish(final, range(tiles // 2, tiles))
    for chunk in chunks:
        for slot in ORDER:
            value_copy(slot, chunk).wait_send()
            grad_copy(slot, chunk).wait_send()


def on_device(
    device_count,
    tracers, mass_flux, lsq_coeff, own_offset, far_offset, inv_mass, neighbour, send_cells,
):
    tracer_count, level_count, cell_count = tracers.shape
    peer_count, halo_width = send_cells.shape
    f32, bf16 = jnp.float32, jnp.bfloat16
    arguments = (
        tracers, mass_flux, lsq_coeff.transpose(1, 0, 2), own_offset, far_offset, inv_mass,
        neighbour, send_cells,
    )
    halo = (peer_count, tracer_count, level_count, halo_width)
    halo_two = (peer_count, tracer_count, 2, level_count, halo_width)
    return pl.pallas_call(
        functools.partial(kernel, device_count),
        out_shape=jax.ShapeDtypeStruct(tracers.shape, f32),
        in_specs=[pl.BlockSpec(memory_space=pltpu.HBM)] * len(arguments),
        out_specs=pl.BlockSpec(memory_space=pltpu.VMEM),
        scratch_shapes=[pltpu.VMEM(a.shape, a.dtype) for a in arguments]
        + [
            pltpu.VMEM(halo, f32),
            pltpu.VMEM(halo, f32),
            pltpu.VMEM(halo_two, f32),
            pltpu.VMEM(halo_two, f32),
            pltpu.VMEM((2, tracer_count, level_count, cell_count), f32),
            pltpu.VMEM((3, tracer_count, level_count, cell_count), f32),
            pltpu.VMEM((3, tracer_count, level_count, cell_count), f32),
            pltpu.VMEM((cell_count, 3 * cell_count), bf16),
            pltpu.VMEM((peer_count * halo_width, 3 * cell_count), bf16),
            pltpu.VMEM((2, tracer_count * level_count, cell_count), bf16),
            pltpu.VMEM((2, tracer_count * 2 * level_count, cell_count), bf16),
            pltpu.VMEM((2, 6 * 2 * level_count, peer_count * halo_width), bf16),
            pltpu.SemaphoreType.DMA((len(arguments),)),
            pltpu.SemaphoreType.DMA((peer_count, len(PARTS))),
            pltpu.SemaphoreType.DMA((peer_count, len(PARTS))),
            pltpu.SemaphoreType.DMA((peer_count, len(PARTS))),
            pltpu.SemaphoreType.DMA((peer_count, len(PARTS))),
        ],
        compiler_params=pltpu.CompilerParams(
            collective_id=0, has_side_effects=True, vmem_limit_bytes=48 * 1024 * 1024
        ),
    )(*[pltpu.with_memory_space_constraint(a, pltpu.HBM) for a in arguments])


def solution(mesh):
    placed = (
        P(None, None, "dom"),
        P(None, None, "dom"),
        P(None, None, "dom"),
        P(None, None, None, "dom"),
        P(None, None, None, "dom"),
        P(None, "dom"),
        P(None, "dom"),
        P(None, "dom"),
    )
    return jax.shard_map(
        functools.partial(on_device, mesh.shape["dom"]),
        mesh=mesh,
        in_specs=placed,
        out_specs=P(None, None, "dom"),
        check_vma=False,
    )
```

```python
import functools

import jax
import jax.numpy as jnp
from jax import lax
from jax.experimental import pallas as pl
from jax.experimental.pallas import tpu as pltpu
from jax.sharding import PartitionSpec as P

LANES = 128
BLOCK = 256
PARTS = (2, 3, 5, 7, 3)
SENT = (2, 3, 5, 7, 3)
JOINED = (((0, 1), 3), ((2,), 3), ((3,), 3), ((4,), 2))
ORDER = (4, 5, 2, 3, 0, 1)


def peer_shift(peer_slot):
    return (peer_slot // 2 + 1) * (1 - 2 * (peer_slot % 2))


def lanes_of(row):
    wide = jnp.broadcast_to(row, (8, LANES))
    return jnp.bitwise_and(wide, LANES - 1), jnp.right_shift(wide, 7)


def taken(tile, lane):
    return jnp.take_along_axis(tile, lane, axis=1, mode="promise_in_bounds")


def in_two(value):
    high = value.astype(jnp.bfloat16)
    return high, (value - high.astype(jnp.float32)).astype(jnp.bfloat16)


def kernel(
    device_count,
    x_any, flux_any, lsq_any, own_any, far_any, inv_any, near_any, send_any,
    result,
    x, flux, lsq, own, far, inv, near, send,
    value_out, value_in, grad_out, grad_in, grad, beside, early,
    own_hot, halo_hot, value_split, grad_split, halo_split,
    load_sem, value_send, value_recv, grad_send, grad_recv,
):
    me = lax.axis_index("dom")
    tracer_count, level_count, cell_count = x.shape
    peer_count = send.shape[0]
    tiles = cell_count // LANES
    starts = [sum(PARTS[:chunk]) for chunk in range(len(PARTS) + 1)]
    cuts = [sum(SENT[:piece]) for piece in range(len(SENT) + 1)]
    targets = [
        lax.rem(me + peer_shift(slot) + device_count, device_count)
        for slot in range(peer_count)
    ]

    barrier = pltpu.get_barrier_semaphore()
    for target in targets:
        pl.semaphore_signal(
            barrier, inc=1, device_id=(target,), device_id_type=pl.DeviceIdType.MESH
        )

    loads = []
    for slot, (source, target) in enumerate((
        (send_any, send), (x_any, x), (near_any, near), (lsq_any, lsq),
        (flux_any, flux), (own_any, own), (far_any, far), (inv_any, inv),
    )):
        copy = pltpu.make_async_copy(source, target, load_sem.at[slot])
        copy.start()
        loads.append(copy)

    def cut(tile):
        return slice(tile * LANES, (tile + 1) * LANES)

    def value_copy(slot, chunk):
        part = pl.ds(starts[chunk], PARTS[chunk])
        return pltpu.make_async_remote_copy(
            src_ref=value_out.at[slot, part],
            dst_ref=value_in.at[slot, part],
            send_sem=value_send.at[slot, chunk],
            recv_sem=value_recv.at[slot, chunk],
            device_id=(targets[slot],),
            device_id_type=pl.DeviceIdType.MESH,
        )

    def grad_copy(slot, piece):
        part = pl.ds(cuts[piece], SENT[piece])
        return pltpu.make_async_remote_copy(
            src_ref=grad_out.at[slot, part],
            dst_ref=grad_in.at[slot, part],
            send_sem=grad_send.at[slot, piece],
            recv_sem=grad_recv.at[slot, piece],
            device_id=(targets[slot],),
            device_id_type=pl.DeviceIdType.MESH,
        )

    def gather_values_to_send(chunk):
        for slot in range(peer_count):
            lane, tile = lanes_of(send[slot : slot + 1, :])
            for t in range(starts[chunk], starts[chunk + 1]):
                found = taken(x[t, :, cut(0)], lane)
                for s in range(1, tiles):
                    found = jnp.where(tile == s, taken(x[t, :, cut(s)], lane), found)
                value_out[slot, t] = found

    def split_values():
        for t in range(0, tracer_count, 2):
            rows = slice(t * level_count, (t + 2) * level_count)
            for c in range(tiles):
                pair = jnp.concatenate([x[t, :, cut(c)], x[t + 1, :, cut(c)]], axis=0)
                for part, half in enumerate(in_two(pair)):
                    value_split[part, rows, cut(c)] = half

    def mark(hot, first):
        depth = hot.shape[0]
        for edge in range(3):
            wanted = (near[edge : edge + 1, :] - first).astype(jnp.int16)
            for k in range(0, depth, 256):
                row = lax.broadcasted_iota(jnp.int16, (256, cell_count), 0) + jnp.int16(k)
                hot[k : k + 256, edge * cell_count : (edge + 1) * cell_count] = jnp.where(
                    row == wanted, jnp.bfloat16(1), jnp.bfloat16(0)
                )

    def gathered(split, rows, hot, edge, block):
        both = jnp.concatenate([split[0, :rows], split[1, :rows]], axis=0)
        first = edge * cell_count + block * BLOCK
        columns = pl.ds(pl.multiple_of(first, BLOCK), BLOCK)
        found = jnp.dot(both, hot[:, columns], preferred_element_type=jnp.float32)
        return found[:rows] + found[rows:]

    def gather_own_values(edge):
        for block in range(cell_count // BLOCK):
            found = gathered(value_split, value_split.shape[1], own_hot, edge, block)
            beside[edge, :, :, slice(block * BLOCK, (block + 1) * BLOCK)] = found.reshape(
                tracer_count, level_count, BLOCK
            )

    def make_gradients(chunk):
        members = range(starts[chunk], starts[chunk + 1])
        for c in range(tiles):
            total = {}
            for edge in range(3):
                lane, tile = lanes_of(near[edge : edge + 1, cut(c)])
                for t in members:
                    found = beside[edge, t, :, cut(c)]
                    for slot in range(peer_count):
                        found = jnp.where(
                            tile == tiles + slot, taken(value_in[slot, t], lane), found
                        )
                    beside[edge, t, :, cut(c)] = found
                    gap = found - x[t, :, cut(c)]
                    for comp in range(2):
                        term = lsq[edge, comp : comp + 1, cut(c)] * gap
                        total[t, comp] = term if edge == 0 else total[t, comp] + term
            for t in members:
                pair = [total[t, comp] for comp in range(2)]
                for comp in range(2):
                    grad[comp, t, :, cut(c)] = pair[comp]
                rows = slice(t * 2 * level_count, (t + 1) * 2 * level_count)
                for part, half in enumerate(in_two(jnp.concatenate(pair, axis=0))):
                    grad_split[part, rows, cut(c)] = half

    def gather_gradients_to_send(chunk):
        for slot in range(peer_count):
            lane, tile = lanes_of(send[slot : slot + 1, :])
            for t in range(starts[chunk], starts[chunk + 1]):
                for comp in range(2):
                    found = taken(grad[comp, t, :, cut(0)], lane)
                    for s in range(1, tiles):
                        found = jnp.where(
                            tile == s, taken(grad[comp, t, :, cut(s)], lane), found
                        )
                    grad_out[slot, t, comp] = found

    def make_early_faces(edge):
        for block in range(cell_count // BLOCK):
            found = gathered(grad_split, grad_split.shape[1], own_hot, edge, block)
            here = slice(block * BLOCK, (block + 1) * BLOCK)
            upwind = flux[edge, :, here] > 0
            for t in range(tracer_count):
                top = t * 2 * level_count
                first = found[top : top + level_count]
                second = found[top + level_count : top + 2 * level_count]
                far_face = (
                    beside[edge, t, :, here]
                    + first * far[0, edge, :, here]
                    + second * far[1, edge, :, here]
                )
                own_face = (
                    x[t, :, here]
                    + grad[0, t, :, here] * own[0, edge, :, here]
                    + grad[1, t, :, here] * own[1, edge, :, here]
                )
                early[edge, t, :, here] = jnp.where(upwind, own_face, far_face)

    def add_halo_faces(first_tracer, count, blocks):
        for inner in range(count):
            rows = slice(inner * 2 * level_count, (inner + 1) * 2 * level_count)
            for slot in range(peer_count):
                pair = grad_in[slot, first_tracer + inner].reshape(2 * level_count, LANES)
                for part, half in enumerate(in_two(pair)):
                    halo_split[part, rows, cut(slot)] = half
        for block in blocks:
            here = slice(block * BLOCK, (block + 1) * BLOCK)
            slopes = [
                gathered(halo_split, count * 2 * level_count, halo_hot, edge, block)
                for edge in range(3)
            ]
            for inner in range(count):
                t = first_tracer + inner
                top = inner * 2 * level_count
                center = x[t, :, here]
                outflow = None
                for edge in range(3):
                    first = slopes[edge][top : top + level_count]
                    second = slopes[edge][top + level_count : top + 2 * level_count]
                    side_flux = flux[edge, :, here]
                    beyond = beside[edge, t, :, here]
                    extra = first * far[0, edge, :, here] + second * far[1, edge, :, here]
                    face = early[edge, t, :, here] + jnp.where(side_flux > 0, 0.0, extra)
                    face = jnp.minimum(
                        jnp.maximum(face, jnp.minimum(center, beyond)),
                        jnp.maximum(center, beyond),
                    )
                    term = side_flux * face
                    outflow = term if edge == 0 else outflow + term
                result[t, :, here] = center - inv[:, here] * outflow

    def finish(first_tracer, count, columns):
        members = range(first_tracer, first_tracer + count)
        for c in columns:
            outflow = {}
            for edge in range(3):
                lane, tile = lanes_of(near[edge : edge + 1, cut(c)])
                side_flux = flux[edge, :, cut(c)]
                late = jnp.logical_and(tile >= tiles, jnp.logical_not(side_flux > 0))
                for t in members:
                    here = x[t, :, cut(c)]
                    beyond = beside[edge, t, :, cut(c)]
                    slopes = []
                    for comp in range(2):
                        found = taken(grad_in[0, t, comp], lane)
                        for slot in range(1, peer_count):
                            found = jnp.where(
                                tile == tiles + slot, taken(grad_in[slot, t, comp], lane), found
                            )
                        slopes.append(found)
                    far_face = (
                        beyond
                        + slopes[0] * far[0, edge, :, cut(c)]
                        + slopes[1] * far[1, edge, :, cut(c)]
                    )
                    face = jnp.where(late, far_face, early[edge, t, :, cut(c)])
                    face = jnp.minimum(
                        jnp.maximum(face, jnp.minimum(here, beyond)), jnp.maximum(here, beyond)
                    )
                    term = side_flux * face
                    outflow[t] = term if edge == 0 else outflow[t] + term
            for t in members:
                result[t, :, cut(c)] = x[t, :, cut(c)] - inv[:, cut(c)] * outflow[t]

    def over(count, body):
        lax.fori_loop(0, count, lambda index, carry: (body(index), carry)[1], 0)

    chunks, pieces = range(len(PARTS)), range(len(SENT))
    loads[0].wait()
    loads[1].wait()
    gather_values_to_send(0)
    pl.semaphore_wait(barrier, peer_count)
    for chunk in chunks:
        if chunk > 0:
            gather_values_to_send(chunk)
        for slot in ORDER:
            value_copy(slot, chunk).start()
    for copy in loads[2:]:
        copy.wait()
    mark(own_hot, 0)
    split_values()
    over(3, gather_own_values)
    for chunk in chunks:
        for slot in ORDER:
            value_copy(slot, chunk).wait_recv()
        make_gradients(chunk)
        gather_gradients_to_send(chunk)
        for piece in pieces:
            if starts[chunk] <= cuts[piece] < starts[chunk + 1]:
                for slot in ORDER:
                    grad_copy(slot, piece).start()
    mark(halo_hot, cell_count)
    over(3, make_early_faces)
    for joined, by_matmul in JOINED:
        for piece in joined:
            for slot in ORDER:
                grad_copy(slot, piece).wait_recv()
        count = sum(SENT[piece] for piece in joined)
        add_halo_faces(cuts[joined[0]], count, range(by_matmul))
        finish(cuts[joined[0]], count, range(by_matmul * BLOCK // LANES, tiles))
    for slot in ORDER:
        for chunk in chunks:
            value_copy(slot, chunk).wait_send()
        for piece in pieces:
            grad_copy(slot, piece).wait_send()


def on_device(
    device_count,
    tracers, mass_flux, lsq_coeff, own_offset, far_offset, inv_mass, neighbour, send_cells,
):
    tracer_count, level_count, cell_count = tracers.shape
    peer_count, halo_width = send_cells.shape
    f32, bf16 = jnp.float32, jnp.bfloat16
    arguments = (
        tracers, mass_flux, lsq_coeff.transpose(1, 0, 2), own_offset, far_offset, inv_mass,
        neighbour, send_cells,
    )
    halo = (peer_count, tracer_count, level_count, halo_width)
    halo_two = (peer_count, tracer_count, 2, level_count, halo_width)
    return pl.pallas_call(
        functools.partial(kernel, device_count),
        out_shape=jax.ShapeDtypeStruct(tracers.shape, f32),
        in_specs=[pl.BlockSpec(memory_space=pltpu.HBM)] * len(arguments),
        out_specs=pl.BlockSpec(memory_space=pltpu.VMEM),
        scratch_shapes=[pltpu.VMEM(a.shape, a.dtype) for a in arguments]
        + [
            pltpu.VMEM(halo, f32),
            pltpu.VMEM(halo, f32),
            pltpu.VMEM(halo_two, f32),
            pltpu.VMEM(halo_two, f32),
            pltpu.VMEM((2, tracer_count, level_count, cell_count), f32),
            pltpu.VMEM((3, tracer_count, level_count, cell_count), f32),
            pltpu.VMEM((3, tracer_count, level_count, cell_count), f32),
            pltpu.VMEM((cell_count, 3 * cell_count), bf16),
            pltpu.VMEM((peer_count * halo_width, 3 * cell_count), bf16),
            pltpu.VMEM((2, tracer_count * level_count, cell_count), bf16),
            pltpu.VMEM((2, tracer_count * 2 * level_count, cell_count), bf16),
            pltpu.VMEM((2, 7 * 2 * level_count, peer_count * halo_width), bf16),
            pltpu.SemaphoreType.DMA((len(arguments),)),
            pltpu.SemaphoreType.DMA((peer_count, len(PARTS))),
            pltpu.SemaphoreType.DMA((peer_count, len(PARTS))),
            pltpu.SemaphoreType.DMA((peer_count, len(SENT))),
            pltpu.SemaphoreType.DMA((peer_count, len(SENT))),
        ],
        compiler_params=pltpu.CompilerParams(
            collective_id=0, has_side_effects=True, vmem_limit_bytes=48 * 1024 * 1024
        ),
    )(*[pltpu.with_memory_space_constraint(a, pltpu.HBM) for a in arguments])


def solution(mesh):
    placed = (
        P(None, None, "dom"),
        P(None, None, "dom"),
        P(None, None, "dom"),
        P(None, None, None, "dom"),
        P(None, None, None, "dom"),
        P(None, "dom"),
        P(None, "dom"),
        P(None, "dom"),
    )
    return jax.shard_map(
        functools.partial(on_device, mesh.shape["dom"]),
        mesh=mesh,
        in_specs=placed,
        out_specs=P(None, None, "dom"),
        check_vma=False,
    )
```

```python
import functools

import jax
import jax.numpy as jnp
from jax import lax
from jax.experimental import pallas as pl
from jax.experimental.pallas import tpu as pltpu
from jax.sharding import PartitionSpec as P

LANES = 128
BLOCK = 256
PARTS = (2, 3, 5, 10)
SENT = (2, 3, 5, 7, 3)
JOINED = (((0, 1), 3), ((2,), 3), ((3,), 3), ((4,), 2))
ORDER = (2, 3, 0, 1, 4, 5)


def peer_shift(peer_slot):
    return (peer_slot // 2 + 1) * (1 - 2 * (peer_slot % 2))


def lanes_of(row):
    wide = jnp.broadcast_to(row, (8, LANES))
    return jnp.bitwise_and(wide, LANES - 1), jnp.right_shift(wide, 7)


def taken(tile, lane):
    return jnp.take_along_axis(tile, lane, axis=1, mode="promise_in_bounds")


def in_two(value):
    high = value.astype(jnp.bfloat16)
    return high, (value - high.astype(jnp.float32)).astype(jnp.bfloat16)


def kernel(
    device_count,
    x_any, flux_any, lsq_any, own_any, far_any, inv_any, near_any, send_any,
    result,
    x, flux, lsq, own, far, inv, near, send,
    value_out, value_in, grad_out, grad_in, grad, beside, early,
    own_hot, halo_hot, value_split, grad_split, halo_split,
    load_sem, value_send, value_recv, grad_send, grad_recv,
):
    me = lax.axis_index("dom")
    tracer_count, level_count, cell_count = x.shape
    peer_count = send.shape[0]
    tiles = cell_count // LANES
    starts = [sum(PARTS[:chunk]) for chunk in range(len(PARTS) + 1)]
    cuts = [sum(SENT[:piece]) for piece in range(len(SENT) + 1)]
    targets = [
        lax.rem(me + peer_shift(slot) + device_count, device_count)
        for slot in range(peer_count)
    ]

    barrier = pltpu.get_barrier_semaphore()
    for target in targets:
        pl.semaphore_signal(
            barrier, inc=1, device_id=(target,), device_id_type=pl.DeviceIdType.MESH
        )

    loads = []
    for slot, (source, target) in enumerate((
        (send_any, send), (x_any, x), (near_any, near), (lsq_any, lsq),
        (flux_any, flux), (own_any, own), (far_any, far), (inv_any, inv),
    )):
        copy = pltpu.make_async_copy(source, target, load_sem.at[slot])
        copy.start()
        loads.append(copy)

    def cut(tile):
        return slice(tile * LANES, (tile + 1) * LANES)

    def value_copy(slot, chunk):
        part = pl.ds(starts[chunk], PARTS[chunk])
        return pltpu.make_async_remote_copy(
            src_ref=value_out.at[slot, part],
            dst_ref=value_in.at[slot, part],
            send_sem=value_send.at[slot, chunk],
            recv_sem=value_recv.at[slot, chunk],
            device_id=(targets[slot],),
            device_id_type=pl.DeviceIdType.MESH,
        )

    def grad_copy(slot, piece):
        part = pl.ds(cuts[piece], SENT[piece])
        return pltpu.make_async_remote_copy(
            src_ref=grad_out.at[slot, part],
            dst_ref=grad_in.at[slot, part],
            send_sem=grad_send.at[slot, piece],
            recv_sem=grad_recv.at[slot, piece],
            device_id=(targets[slot],),
            device_id_type=pl.DeviceIdType.MESH,
        )

    def gather_values_to_send(chunk):
        for slot in range(peer_count):
            lane, tile = lanes_of(send[slot : slot + 1, :])
            for t in range(starts[chunk], starts[chunk + 1]):
                found = taken(x[t, :, cut(0)], lane)
                for s in range(1, tiles):
                    found = jnp.where(tile == s, taken(x[t, :, cut(s)], lane), found)
                value_out[slot, t] = found

    def split_values():
        for t in range(0, tracer_count, 2):
            rows = slice(t * level_count, (t + 2) * level_count)
            for c in range(tiles):
                pair = jnp.concatenate([x[t, :, cut(c)], x[t + 1, :, cut(c)]], axis=0)
                for part, half in enumerate(in_two(pair)):
                    value_split[part, rows, cut(c)] = half

    def mark(hot, first):
        depth = hot.shape[0]
        for edge in range(3):
            wanted = (near[edge : edge + 1, :] - first).astype(jnp.int16)
            for k in range(0, depth, 256):
                row = lax.broadcasted_iota(jnp.int16, (256, cell_count), 0) + jnp.int16(k)
                hot[k : k + 256, edge * cell_count : (edge + 1) * cell_count] = jnp.where(
                    row == wanted, jnp.bfloat16(1), jnp.bfloat16(0)
                )

    def gathered(split, rows, hot, edge, block):
        both = jnp.concatenate([split[0, :rows], split[1, :rows]], axis=0)
        first = edge * cell_count + block * BLOCK
        columns = pl.ds(pl.multiple_of(first, BLOCK), BLOCK)
        found = jnp.dot(both, hot[:, columns], preferred_element_type=jnp.float32)
        return found[:rows] + found[rows:]

    def gather_own_values(edge):
        for block in range(cell_count // BLOCK):
            found = gathered(value_split, value_split.shape[1], own_hot, edge, block)
            beside[edge, :, :, slice(block * BLOCK, (block + 1) * BLOCK)] = found.reshape(
                tracer_count, level_count, BLOCK
            )

    def make_gradients(chunk):
        members = range(starts[chunk], starts[chunk + 1])
        for c in range(tiles):
            total = {}
            for edge in range(3):
                lane, tile = lanes_of(near[edge : edge + 1, cut(c)])
                for t in members:
                    found = beside[edge, t, :, cut(c)]
                    for slot in range(peer_count):
                        found = jnp.where(
                            tile == tiles + slot, taken(value_in[slot, t], lane), found
                        )
                    beside[edge, t, :, cut(c)] = found
                    gap = found - x[t, :, cut(c)]
                    for comp in range(2):
                        term = lsq[edge, comp : comp + 1, cut(c)] * gap
                        total[t, comp] = term if edge == 0 else total[t, comp] + term
            for t in members:
                pair = [total[t, comp] for comp in range(2)]
                for comp in range(2):
                    grad[comp, t, :, cut(c)] = pair[comp]
                rows = slice(t * 2 * level_count, (t + 1) * 2 * level_count)
                for part, half in enumerate(in_two(jnp.concatenate(pair, axis=0))):
                    grad_split[part, rows, cut(c)] = half

    def gather_gradients_to_send(chunk):
        for slot in range(peer_count):
            lane, tile = lanes_of(send[slot : slot + 1, :])
            for t in range(starts[chunk], starts[chunk + 1]):
                for comp in range(2):
                    found = taken(grad[comp, t, :, cut(0)], lane)
                    for s in range(1, tiles):
                        found = jnp.where(
                            tile == s, taken(grad[comp, t, :, cut(s)], lane), found
                        )
                    grad_out[slot, t, comp] = found

    def make_early_faces(edge):
        for block in range(cell_count // BLOCK):
            found = gathered(grad_split, grad_split.shape[1], own_hot, edge, block)
            here = slice(block * BLOCK, (block + 1) * BLOCK)
            upwind = flux[edge, :, here] > 0
            for t in range(tracer_count):
                top = t * 2 * level_count
                first = found[top : top + level_count]
                second = found[top + level_count : top + 2 * level_count]
                far_face = (
                    beside[edge, t, :, here]
                    + first * far[0, edge, :, here]
                    + second * far[1, edge, :, here]
                )
                own_face = (
                    x[t, :, here]
                    + grad[0, t, :, here] * own[0, edge, :, here]
                    + grad[1, t, :, here] * own[1, edge, :, here]
                )
                early[edge, t, :, here] = jnp.where(upwind, own_face, far_face)

    def add_halo_faces(first_tracer, count, blocks):
        for inner in range(count):
            rows = slice(inner * 2 * level_count, (inner + 1) * 2 * level_count)
            for slot in range(peer_count):
                pair = grad_in[slot, first_tracer + inner].reshape(2 * level_count, LANES)
                for part, half in enumerate(in_two(pair)):
                    halo_split[part, rows, cut(slot)] = half
        for block in blocks:
            here = slice(block * BLOCK, (block + 1) * BLOCK)
            slopes = [
                gathered(halo_split, count * 2 * level_count, halo_hot, edge, block)
                for edge in range(3)
            ]
            for inner in range(count):
                t = first_tracer + inner
                top = inner * 2 * level_count
                center = x[t, :, here]
                outflow = None
                for edge in range(3):
                    first = slopes[edge][top : top + level_count]
                    second = slopes[edge][top + level_count : top + 2 * level_count]
                    side_flux = flux[edge, :, here]
                    beyond = beside[edge, t, :, here]
                    extra = first * far[0, edge, :, here] + second * far[1, edge, :, here]
                    face = early[edge, t, :, here] + jnp.where(side_flux > 0, 0.0, extra)
                    face = jnp.minimum(
                        jnp.maximum(face, jnp.minimum(center, beyond)),
                        jnp.maximum(center, beyond),
                    )
                    term = side_flux * face
                    outflow = term if edge == 0 else outflow + term
                result[t, :, here] = center - inv[:, here] * outflow

    def finish(first_tracer, count, columns):
        members = range(first_tracer, first_tracer + count)
        for c in columns:
            outflow = {}
            for edge in range(3):
                lane, tile = lanes_of(near[edge : edge + 1, cut(c)])
                side_flux = flux[edge, :, cut(c)]
                late = jnp.logical_and(tile >= tiles, jnp.logical_not(side_flux > 0))
                for t in members:
                    here = x[t, :, cut(c)]
                    beyond = beside[edge, t, :, cut(c)]
                    slopes = []
                    for comp in range(2):
                        found = taken(grad_in[0, t, comp], lane)
                        for slot in range(1, peer_count):
                            found = jnp.where(
                                tile == tiles + slot, taken(grad_in[slot, t, comp], lane), found
                            )
                        slopes.append(found)
                    far_face = (
                        beyond
                        + slopes[0] * far[0, edge, :, cut(c)]
                        + slopes[1] * far[1, edge, :, cut(c)]
                    )
                    face = jnp.where(late, far_face, early[edge, t, :, cut(c)])
                    face = jnp.minimum(
                        jnp.maximum(face, jnp.minimum(here, beyond)), jnp.maximum(here, beyond)
                    )
                    term = side_flux * face
                    outflow[t] = term if edge == 0 else outflow[t] + term
            for t in members:
                result[t, :, cut(c)] = x[t, :, cut(c)] - inv[:, cut(c)] * outflow[t]

    def over(count, body):
        lax.fori_loop(0, count, lambda index, carry: (body(index), carry)[1], 0)

    chunks, pieces = range(len(PARTS)), range(len(SENT))
    loads[0].wait()
    loads[1].wait()
    gather_values_to_send(0)
    pl.semaphore_wait(barrier, peer_count)
    for chunk in chunks:
        if chunk > 0:
            gather_values_to_send(chunk)
        for slot in ORDER:
            value_copy(slot, chunk).start()
    for copy in loads[2:]:
        copy.wait()
    mark(own_hot, 0)
    split_values()
    over(3, gather_own_values)
    for chunk in chunks:
        for slot in ORDER:
            value_copy(slot, chunk).wait_recv()
        make_gradients(chunk)
        gather_gradients_to_send(chunk)
        for piece in pieces:
            if starts[chunk] <= cuts[piece] < starts[chunk + 1]:
                for slot in ORDER:
                    grad_copy(slot, piece).start()
    mark(halo_hot, cell_count)
    over(3, make_early_faces)
    for joined, by_matmul in JOINED:
        for piece in joined:
            for slot in ORDER:
                grad_copy(slot, piece).wait_recv()
        count = sum(SENT[piece] for piece in joined)
        add_halo_faces(cuts[joined[0]], count, range(by_matmul))
        finish(cuts[joined[0]], count, range(by_matmul * BLOCK // LANES, tiles))
    for slot in ORDER:
        for chunk in chunks:
            value_copy(slot, chunk).wait_send()
        for piece in pieces:
            grad_copy(slot, piece).wait_send()


def on_device(
    device_count,
    tracers, mass_flux, lsq_coeff, own_offset, far_offset, inv_mass, neighbour, send_cells,
):
    tracer_count, level_count, cell_count = tracers.shape
    peer_count, halo_width = send_cells.shape
    f32, bf16 = jnp.float32, jnp.bfloat16
    arguments = (
        tracers, mass_flux, lsq_coeff.transpose(1, 0, 2), own_offset, far_offset, inv_mass,
        neighbour, send_cells,
    )
    halo = (peer_count, tracer_count, level_count, halo_width)
    halo_two = (peer_count, tracer_count, 2, level_count, halo_width)
    return pl.pallas_call(
        functools.partial(kernel, device_count),
        out_shape=jax.ShapeDtypeStruct(tracers.shape, f32),
        in_specs=[pl.BlockSpec(memory_space=pltpu.HBM)] * len(arguments),
        out_specs=pl.BlockSpec(memory_space=pltpu.VMEM),
        scratch_shapes=[pltpu.VMEM(a.shape, a.dtype) for a in arguments]
        + [
            pltpu.VMEM(halo, f32),
            pltpu.VMEM(halo, f32),
            pltpu.VMEM(halo_two, f32),
            pltpu.VMEM(halo_two, f32),
            pltpu.VMEM((2, tracer_count, level_count, cell_count), f32),
            pltpu.VMEM((3, tracer_count, level_count, cell_count), f32),
            pltpu.VMEM((3, tracer_count, level_count, cell_count), f32),
            pltpu.VMEM((cell_count, 3 * cell_count), bf16),
            pltpu.VMEM((peer_count * halo_width, 3 * cell_count), bf16),
            pltpu.VMEM((2, tracer_count * level_count, cell_count), bf16),
            pltpu.VMEM((2, tracer_count * 2 * level_count, cell_count), bf16),
            pltpu.VMEM((2, 7 * 2 * level_count, peer_count * halo_width), bf16),
            pltpu.SemaphoreType.DMA((len(arguments),)),
            pltpu.SemaphoreType.DMA((peer_count, len(PARTS))),
            pltpu.SemaphoreType.DMA((peer_count, len(PARTS))),
            pltpu.SemaphoreType.DMA((peer_count, len(SENT))),
            pltpu.SemaphoreType.DMA((peer_count, len(SENT))),
        ],
        compiler_params=pltpu.CompilerParams(
            collective_id=0, has_side_effects=True, vmem_limit_bytes=48 * 1024 * 1024
        ),
    )(*[pltpu.with_memory_space_constraint(a, pltpu.HBM) for a in arguments])


def solution(mesh):
    placed = (
        P(None, None, "dom"),
        P(None, None, "dom"),
        P(None, None, "dom"),
        P(None, None, None, "dom"),
        P(None, None, None, "dom"),
        P(None, "dom"),
        P(None, "dom"),
        P(None, "dom"),
    )
    return jax.shard_map(
        functools.partial(on_device, mesh.shape["dom"]),
        mesh=mesh,
        in_specs=placed,
        out_specs=P(None, None, "dom"),
        check_vma=False,
    )
```
